32 devices in a mesh: px: 4 (over y, x), py: 8 (over z, core).
Axes of the slice: x: 2, y: 2, z: 4, core: 2. Of those that a mesh axis runs over, the one named last changes fastest.
Arguments:
- photons: float32 [1024, 128], P(('px', 'py')), may hold values from 50 to 1000
- halo_cells: int32 [1024, 128], P(('px', 'py')), may hold values from 0 to 1769471
- halo_counts: int32 [1024], P(('px', 'py')), may hold values from 1 to 128
- owners: int32 [1024, 1], P(('px', 'py')), may hold values from 0 to 7; in each aligned block of 32 rows (0 to 31, 32 to 63, ...) at most 4 rows name the same one
- density: float32 [384, 384, 384], P('px', 'py'), may hold values from 0.02 to 50
Outputs:
- fraction: float32 [384, 384, 384], P('px', 'py')
The draws below stay inside these ranges and needn't reach their ends.
Inputs may be any that keep to these rules, and one draw needn't show every extreme that they name: The halos of a block all lie in pencil owners[b] of the block's own slab. Among the 32 blocks of one device no owner appears more than 4 times, a bound that some block reaches. Slots at or past halo_counts[b] are not live and carry arbitrary values. `halo_cells`: A cell index within the owner pencil is (x * 48 + y) * 384 + z with x, y, z local to that pencil.
All inputs are finite; a program needn't handle non-finite values.
Results may differ from the reference program's by a relative error of at most 0.0003.
Values sent between devices are 32-bit elements; how exact they have to be, the bound alone decides.
A program may use at most 192 MiB of HBM per device.

```python
import math
import jax
import jax.numpy as jnp
import numpy as np
from jax import lax

NG = 384
SLOTS = 128
CAP = 4
RADIUS = 20
BLK_DEV = 32
CX = 96
CY = 48
HROWS = 1024
N_PY = 8


def draw_density(key, part):
    subkeys = jax.random.split(jax.random.fold_in(key, 7), 4)
    wave_numbers = jax.random.randint(subkeys[0], (4, 3), 1, 4)
    flip_signs = jax.random.randint(subkeys[1], (4, 3), 0, 2) * 2 - 1
    wave_numbers = wave_numbers * flip_signs
    phases = jax.random.uniform(subkeys[2], (4,), jnp.float32, -jnp.pi, jnp.pi)
    coords = jnp.arange(NG, dtype=jnp.int32)
    smooth = jnp.zeros((NG, NG, NG), jnp.float32)
    for number in range(4):
        along_x = wave_numbers[number, 0] * coords % NG
        along_y = wave_numbers[number, 1] * coords % NG
        along_z = wave_numbers[number, 2] * coords % NG
        total = (along_x[:, None, None] + along_y[None, :, None] + along_z[None, None, :]) % NG
        smooth = smooth + jnp.cos(total.astype(jnp.float32) * (2.0 * jnp.pi / NG) + phases[number])
    smooth = smooth / jnp.sqrt(2.0)
    rough_part = jnp.clip(1.8 * jax.random.normal(subkeys[3], (NG, NG, NG), jnp.float32), -4.0, 4.0) - 1.4
    amplitude = 0.8
    return jnp.clip(jnp.exp(amplitude * smooth + rough_part), 0.02, 50.0).astype(jnp.float32)


def place_ends(result, own_key, smallest, top_value):
    spot = [jax.random.randint(jax.random.fold_in(own_key, axis), (), 0, length) for axis, length in enumerate(result.shape)]
    main_axis = result.shape.index(max(result.shape))
    neighbour = spot[:main_axis] + [(spot[main_axis] + 1) % result.shape[main_axis]] + spot[main_axis + 1:]
    return result.at[tuple(spot)].set(smallest).at[tuple(neighbour)].set(top_value)


def level_of(key, extent, pieces, low, largest):
    factor_of = 1.0
    for axis_at, shards_of in pieces:
        heights = jax.random.uniform(jax.random.fold_in(jax.random.fold_in(key, 6), axis_at), (shards_of,), jnp.float32, low / len(pieces), largest / len(pieces))
        factor_of = factor_of * jnp.repeat(jnp.exp(heights), extent[axis_at] // shards_of).reshape((-1,) + (1,) * (len(extent) - 1 - axis_at))
    return factor_of


def deal_out(stream_key, own, number, rows, amount, top, most, skew):
    sequence = jax.random.permutation(stream_key, amount)
    crowded, usual = shares(amount, rows * top, most, skew, True), shares(amount, rows * top, most, skew, False)
    places = jnp.arange(amount)

    def named(sizes, rotation):
        used = int((sizes > 0).sum())
        fixed = max(1, used // 4)
        passed = fixed + (places - fixed + rotation * (used - fixed)) % max(1, amount - fixed)
        return jnp.zeros((amount,), jnp.int32).at[sequence[jnp.where(places < fixed, places, passed)]].set(jnp.asarray(sizes, jnp.int32))

    sizes = jnp.where(number % 4 == 0, named(crowded, number // 4), named(usual, number - number // 4 - 1))
    mixed = jax.random.permutation(jax.random.fold_in(own, 3), amount)
    giver, receiver = mixed[0:amount // 2 * 2:2], mixed[1:amount // 2 * 2:2]
    margin = jnp.minimum(sizes[giver] - 1, most - sizes[receiver]) // 2
    margin = jnp.where((giver == sequence[0]) | (receiver == sequence[0]) | (sizes[receiver] == 0), 0, jnp.maximum(margin, 0))
    passed = jax.random.randint(jax.random.fold_in(own, 4), (amount // 2,), 0, 1 << 20) % (margin + 1)
    sizes = sizes.at[giver].add(-passed).at[receiver].add(passed)
    items = jnp.searchsorted(jnp.cumsum(sizes), jnp.arange(rows * top), side="right").astype(jnp.int32)
    table = items.reshape(top, rows).T
    table = table[jax.random.permutation(jax.random.fold_in(own, 1), rows)]
    rotation = jax.random.randint(jax.random.fold_in(own, 2), (rows, 1), 0, top)
    return jnp.take_along_axis(table, (jnp.arange(top)[None, :] + rotation) % top, axis=1)


def shares(count, total, reach, slope, full):
    weights = [(1 << 20) // math.isqrt(rank ** slope) + 1 for rank in range(1, count + 1)]
    largest = reach if full else min(reach, max(-(-total // count), total * weights[0] // sum(weights)))
    least = 1 if total - largest >= count - 1 else 0
    counts, spare = [largest] + [least] * (count - 1), total - largest - least * (count - 1)
    while spare > 0:
        free = [i for i in range(1, count) if counts[i] < largest] or [i for i in range(1, count) if counts[i] < reach]
        whole, budget = sum([weights[i] for i in free]), spare
        for i in free:
            extra = min(reach - counts[i], max(1, budget * weights[i] // whole), spare)
            counts[i] = counts[i] + extra
            spare = spare - extra
    return np.array(counts)


def setup_inputs(seed: int = 0) -> dict:
    seeds = jax.random.split(jax.random.key(seed), 6)
    photons = jnp.clip(jnp.exp(math.log(1000.0) - 2.9957323 * jax.random.uniform(seeds[0], (HROWS, SLOTS), jnp.float32) ** level_of(seeds[0], (HROWS, SLOTS), ((0, 32),), -0.2, 0.2)), 50.0, 1000.0)
    halo_cells = place_ends(jax.random.randint(seeds[1], (HROWS, SLOTS), 0, CX * CY * NG), jax.random.fold_in(seeds[1], 1), 0, (CX * CY * NG) - 1).astype(jnp.int32)
    halo_counts = place_ends(jax.random.randint(seeds[2], (HROWS,), 1, SLOTS + 1), jax.random.fold_in(seeds[2], 1), 1, SLOTS).astype(jnp.int32)
    owners_keys = jax.random.split(jax.random.fold_in(seeds[3], 1), HROWS // BLK_DEV)
    owners_turns = jax.random.permutation(jax.random.fold_in(seeds[3], 3), HROWS // BLK_DEV)
    owners = jax.vmap(lambda own, number: deal_out(jax.random.fold_in(seeds[3], 2), own, number, BLK_DEV, N_PY, 1, CAP, 2))(owners_keys, owners_turns).reshape((HROWS, 1))
    density = draw_density(jax.random.fold_in(seeds[5], 71), 0)
    return dict(photons=photons, halo_cells=halo_cells, halo_counts=halo_counts, owners=owners, density=density)


def top_hat(freq_x, freq_y, freq_z):
    radial = jnp.sqrt(freq_x * freq_x + freq_y * freq_y + freq_z * freq_z) * (2.0 * jnp.pi * RADIUS / NG)
    safe = jnp.where(radial > 0, radial, 1.0)
    value = 3.0 * (jnp.sin(safe) - safe * jnp.cos(safe)) / (safe * safe * safe)
    return jnp.where(radial > 0, value, 1.0)

def reference(photons, halo_cells, halo_counts, owners, density):
    row_count = photons.shape[0]
    row_index = jnp.arange(row_count, dtype=jnp.int32)
    slab_index = row_index // (N_PY * BLK_DEV)
    local_x = halo_cells // (CY * NG)
    local_y = halo_cells // NG % CY
    local_z = halo_cells % NG
    global_x = slab_index[:, None] * CX + local_x
    global_y = owners[:, 0:1] * CY + local_y
    flat_index = ((global_x * NG + global_y) * NG + local_z).astype(jnp.int32)
    live_slots = jnp.arange(photons.shape[1], dtype=jnp.int32)[None, :] < halo_counts[:, None]
    weights = jnp.where(live_slots, photons, jnp.zeros_like(photons))
    field = jnp.zeros((NG * NG * NG,), photons.dtype).at[flat_index.reshape(-1)].add(weights.reshape(-1))
    field = field.reshape(NG, NG, NG)
    packed = lax.complex(field, density)
    spectrum = jnp.fft.fftn(packed)
    index_values = jnp.arange(NG, dtype=jnp.int32)
    signed_frequency = jnp.where(index_values < NG // 2, index_values, index_values - NG).astype(density.dtype)
    window = top_hat(signed_frequency[:, None, None], signed_frequency[None, :, None], signed_frequency[None, None, :])
    smoothed = jnp.fft.ifftn(spectrum * window)
    photon_smooth = jnp.real(smoothed)
    density_smooth = jnp.imag(smoothed)
    fraction = jnp.clip(photon_smooth / jnp.maximum(density_smooth, 0.5), 0.0, 1.0)
    return fraction.astype(jnp.float32)
```

```python
import jax
import jax.numpy as jnp
import numpy as np
from jax import lax
from jax.sharding import PartitionSpec as P

CAP = 4
RADIUS = 20
LANES = 128


def product(form, left, right):
    return jnp.einsum(form, left, right, precision=lax.Precision.HIGH)


def hartley(length):
    index_row = np.arange(length)
    angle = (index_row[:, None] * index_row[None, :] % length) * (2.0 * np.pi / length)
    return ((np.cos(angle) + np.sin(angle)) / np.sqrt(length)).astype(np.float32)


def top_hat(freq_x, freq_y, freq_z, grid):
    radial = jnp.sqrt(freq_x * freq_x + freq_y * freq_y + freq_z * freq_z) * (
        2.0 * jnp.pi * RADIUS / grid
    )
    safe = jnp.where(radial > 0, radial, 1.0)
    value = 3.0 * (jnp.sin(safe) - safe * jnp.cos(safe)) / (safe * safe * safe)
    return jnp.where(radial > 0, value, 1.0)


def on_device(photons, halo_cells, halo_counts, owners, density):
    rows_x, rows_y, grid = density.shape
    blocks, slots = photons.shape
    count_x = lax.axis_size("px")
    count_y = lax.axis_size("py")
    place_y = lax.axis_index("py")
    devices_all = count_x * count_y
    planes = grid // devices_all
    area = rows_x * rows_y
    table = jnp.asarray(hartley(grid))
    table_x = table.reshape(count_x, rows_x, grid)
    table_y = table.reshape(count_y, rows_y, grid)

    assert area * grid < 1 << 24
    slot_index = jnp.arange(slots, dtype=jnp.int32)[None, :]
    weights = jnp.where(slot_index < halo_counts[:, None], photons, 0.0)
    row = halo_cells // grid
    spot = ((row % rows_y) * rows_x + row // rows_y) * grid + halo_cells % grid
    owner_row = jnp.broadcast_to(owners, (blocks, slots))
    sent = jnp.stack([weights, spot.astype(jnp.float32), owner_row.astype(jnp.float32)])
    slab = lax.all_gather(sent, "py", axis=1, tiled=True)
    slab, density = lax.optimization_barrier((slab, density))

    def signed(index_values):
        return jnp.where(index_values < grid // 2, index_values, index_values - grid).astype(
            jnp.float32
        )

    def exchange(blocks_out):
        got = lax.all_to_all(
            blocks_out.reshape(devices_all, planes * area // LANES, LANES),
            ("px", "py"), split_axis=0, concat_axis=0, tiled=True,
        )
        return got

    def forward(field_rows):
        spec = product("az,zk->ka", field_rows, table)
        return exchange(spec)

    def middle(got):
        got = got.reshape(count_x, count_y, planes, rows_y, rows_x)
        half = product("iqklx,ixn->qkln", got, table_x)
        full = product("qkln,qlm->kmn", half, table_y) * window
        half = product("kmn,qlm->qkln", full, table_y)
        back = product("qkln,ixn->iqklx", half, table_x)
        return exchange(back)

    def backward(got):
        return product("ka,kz->az", got.reshape(grid, area), table)

    density_rows = density.transpose(1, 0, 2).reshape(area, grid)
    density_spec = forward(density_rows)

    freq = signed(jnp.arange(grid, dtype=jnp.int32))
    freq_z = signed(
        lax.axis_index(("px", "py")) * planes + jnp.arange(planes, dtype=jnp.int32)
    )
    window = top_hat(freq_z[:, None, None], freq[None, :, None], freq[None, None, :], grid)
    window = lax.optimization_barrier(window)

    owned = slab[2, :, 0] == place_y.astype(jnp.float32)
    chosen = jnp.argsort(jnp.where(owned, 0, 1), stable=True)[: CAP * count_y]
    own_weights = jnp.where(owned[chosen][:, None], slab[0][chosen], 0.0)
    own_spot = slab[1][chosen].astype(jnp.int32)
    painted = jnp.zeros((area * grid,), jnp.float32)
    painted = painted.at[own_spot.reshape(-1)].add(own_weights.reshape(-1))
    photon_spec = forward(painted.reshape(area, grid))

    density_smooth = backward(middle(density_spec))
    photon_smooth = backward(middle(photon_spec))

    fraction = jnp.clip(photon_smooth / jnp.maximum(density_smooth, 0.5), 0.0, 1.0)
    return fraction.reshape(rows_y, rows_x, grid).transpose(1, 0, 2)


def solution(mesh):
    placed = (
        P(("px", "py"), None),
        P(("px", "py"), None),
        P(("px", "py")),
        P(("px", "py"), None),
        P("px", "py", None),
    )
    return jax.shard_map(
        on_device, mesh=mesh, in_specs=placed, out_specs=P("px", "py", None), check_vma=False
    )
```

```python
import jax
import jax.numpy as jnp
import numpy as np
from jax import lax
from jax.experimental import pallas as pl
from jax.experimental.pallas import tpu as pltpu
from jax.sharding import PartitionSpec as P

RADIUS = 20
LANES = 128
UNROLL = 8
TAB_BITS = 10


def product(form, left, right):
    return jnp.einsum(form, left, right, precision=lax.Precision.HIGH)


def hartley(length):
    index_row = np.arange(length)
    angle = (index_row[:, None] * index_row[None, :] % length) * (2.0 * np.pi / length)
    return ((np.cos(angle) + np.sin(angle)) / np.sqrt(length)).astype(np.float32)


def sine_cosine(angle):
    turns = jnp.round(angle * np.float32(2.0 / np.pi))
    rest = angle - turns * np.float32(1.5703125)
    rest = rest - turns * np.float32(4.837512969970703e-4)
    rest = rest - turns * np.float32(7.549789948768648e-8)
    square = rest * rest
    sine = ((-1.9515295891e-4 * square + 8.3321608736e-3) * square - 1.6666654611e-1) * (
        square * rest
    ) + rest
    cosine = (
        (2.443315711809948e-5 * square - 1.388731625493765e-3) * square + 4.166664568298827e-2
    ) * (square * square) + (1.0 - 0.5 * square)
    quarter = turns.astype(jnp.int32)
    swap = (quarter & 1) == 1
    first, second = jnp.where(swap, cosine, sine), jnp.where(swap, sine, cosine)
    first = jnp.where((quarter & 2) == 2, -first, first)
    second = jnp.where(((quarter + 1) & 2) == 2, -second, second)
    return first, second


def top_hat(freq_x, freq_y, freq_z, grid):
    radial = jnp.sqrt(freq_x * freq_x + freq_y * freq_y + freq_z * freq_z) * (
        2.0 * jnp.pi * RADIUS / grid
    )
    safe = jnp.where(radial > 0, radial, 1.0)
    sine, cosine = sine_cosine(safe)
    value = 3.0 * (sine - safe * cosine) / (safe * safe * safe)
    return jnp.where(radial > 0, value, 1.0)


def paint_kernel(key, weight, count, waves, out, other):
    rows = out.shape[0]
    step = 256
    sums = (out, other)

    @pl.loop(0, rows // step)
    def _(index):
        part = pl.ds(pl.multiple_of(index * step, step), step)
        for total in sums:
            total[part, :] = jnp.zeros((step, LANES), jnp.float32)

    @pl.loop(0, key.shape[0])
    def _(block):
        turns = lax.div(count[block] + (UNROLL - 1), UNROLL)

        @pl.loop(0, turns)
        def _(turn):
            for lane in range(UNROLL):
                slot = turn * UNROLL + lane
                both = key[block, slot]
                row = pl.ds(lax.shift_right_logical(both, TAB_BITS), 1)
                wave = pl.ds(lax.bitwise_and(both, (1 << TAB_BITS) - 1), 1)
                total = sums[lane % len(sums)]
                total[row, :] = total[row, :] + weight[block, slot] * waves[wave, :]

    @pl.loop(0, rows // step)
    def _(index):
        part = pl.ds(pl.multiple_of(index * step, step), step)
        out[part, :] = out[part, :] + other[part, :]


def paint(key, weight, count, waves, rows):
    smem = pl.BlockSpec(memory_space=pltpu.SMEM)
    vmem = pl.BlockSpec(memory_space=pltpu.VMEM)
    return pl.pallas_call(
        paint_kernel,
        out_shape=jax.ShapeDtypeStruct((rows, LANES), jnp.float32),
        in_specs=[smem, smem, smem, vmem],
        out_specs=vmem,
        scratch_shapes=[pltpu.VMEM((rows, LANES), jnp.float32)],
        cost_estimate=pl.CostEstimate(
            flops=80_000_000_000, bytes_accessed=rows * LANES * 4, transcendentals=0
        ),
        compiler_params=pltpu.CompilerParams(vmem_limit_bytes=3 * rows * LANES * 4),
        name="paint",
    )(key, weight, count, waves)


def on_device(photons, halo_cells, halo_counts, owners, density):
    rows_x, rows_y, grid = density.shape
    slots = photons.shape[1]
    count_x = lax.axis_size("px")
    count_y = lax.axis_size("py")
    place_x = lax.axis_index("px")
    place_y = lax.axis_index("py")
    devices_all = count_x * count_y
    planes = grid // devices_all
    area = rows_x * rows_y
    table_np = hartley(grid)
    table = jnp.asarray(table_np)
    table_x = table.reshape(count_x, rows_x, grid)
    table_y = table.reshape(count_y, rows_y, grid)

    first = max(1, planes * 2 // 3)
    parts = [(0, first)] + ([(first, planes)] if first < planes else [])
    by_plane = table_np.reshape(grid, devices_all, planes)
    tables = [
        jnp.asarray(np.ascontiguousarray(by_plane[:, :, a:b]).reshape(grid, devices_all * (b - a)))
        for a, b in parts
    ]

    pair = LANES // 2
    width = pair // count_x
    assert planes <= width and rows_x % 2 == 0
    assert 2 * grid <= 1 << TAB_BITS and rows_x * grid * grid < 1 << 24
    half_x = rows_x // 2
    rows = grid * half_x
    slot_index = jnp.arange(slots, dtype=jnp.int32)[None, :]
    live = slot_index < halo_counts[:, None]
    weights = jnp.where(live, photons, 0.0)
    cell_x = halo_cells // (rows_y * grid)
    cell_y = owners * rows_y + halo_cells // grid % rows_y
    cell_z = halo_cells % grid
    row = (cell_x // 2) * grid + cell_y
    key = jnp.where(live, row * (2 * grid) + (cell_x % 2) * grid + cell_z, 0)
    sent = jnp.stack([weights, key.astype(jnp.float32)])
    slab = lax.all_gather(sent, "py", axis=1, tiled=True)
    slab, density = lax.optimization_barrier((slab, density))

    def signed(index_values):
        return jnp.where(index_values < grid // 2, index_values, index_values - grid).astype(
            jnp.float32
        )

    received = []

    def exchange(blocks_out):
        blocks_out = blocks_out.reshape(devices_all, -1, LANES)
        if received:
            blocks_out, _ = lax.optimization_barrier((blocks_out, received[-1]))
        got = lax.all_to_all(
            blocks_out, ("px", "py"), split_axis=0, concat_axis=0, tiled=True
        )
        received.append(got)
        return got

    density_rows = density.transpose(1, 0, 2).reshape(area, grid)
    specs = [product("az,zk->ka", density_rows, part) for part in tables]
    density_got = [exchange(specs[0])]

    freq = signed(jnp.arange(grid, dtype=jnp.int32))
    freq_z = signed(
        lax.axis_index(("px", "py")) * planes + jnp.arange(planes, dtype=jnp.int32)
    )
    windows = [
        lax.optimization_barrier(
            top_hat(freq_z[a:b, None, None], freq[None, :, None], freq[None, None, :], grid)
        )
        for a, b in parts
    ]

    all_keys = slab[1].astype(jnp.int32)
    all_keys = all_keys // (2 * grid) * (1 << TAB_BITS) + all_keys % (2 * grid)
    all_counts = jnp.max(jnp.where(slab[0] != 0.0, slot_index + 1, 0), axis=1)
    own = lax.dynamic_index_in_dim(
        table.reshape(grid, count_x, count_y, planes), place_y, 2, keepdims=False
    )
    own = jnp.pad(own, ((0, 0), (0, 0), (0, width - planes))).reshape(grid, pair)
    waves = jnp.concatenate(
        [jnp.pad(own, ((0, 0), (0, pair))), jnp.pad(own, ((0, 0), (pair, 0)))]
    )
    painted = paint(all_keys, slab[0], all_counts, waves, rows)
    for spec in specs[1:]:
        spec, painted, windows[0] = lax.optimization_barrier((spec, painted, windows[0]))
        density_got.append(exchange(spec))

    def outward(full):
        half = product("kmn,qlm->qkln", full, table_y)
        back = product("qkln,ixn->iqklx", half, table_x)
        return exchange(back)

    def inward(got):
        got = got.reshape(count_x, count_y, -1, rows_y, rows_x)
        half = product("iqklx,ixn->qkln", got, table_x)
        return product("qkln,qlm->kmn", half, table_y)

    lines = product("ayc,ym->acm", painted.reshape(half_x, grid, LANES), table)
    lines = lines.reshape(rows_x, count_x, width, grid)[:, :, :planes]
    lines = lines.transpose(1, 2, 0, 3)
    rows_of = [
        lax.dynamic_index_in_dim(table_x, (place_x - shift) % count_x, 0, keepdims=False)
        for shift in range(count_x)
    ]
    photon_parts = [
        [
            lax.dynamic_slice(
                lines, ((place_x + shift) % count_x, a, 0, 0), (1, b - a, rows_x, grid)
            )[0]
            for shift in range(count_x)
        ]
        for a, b in parts
    ]

    def around(block, shift):
        if shift == 0:
            return block
        return lax.ppermute(block, "px", [(i, (i + shift) % count_x) for i in range(count_x)])

    photon_parts = [
        [around(block, shift) for shift, block in enumerate(blocks)]
        for blocks in photon_parts
    ]

    def crosswise(blocks):
        total = None
        for block, rows_from in zip(blocks, rows_of):
            term = product("kxm,xn->kmn", block, rows_from)
            total = term if total is None else total + term
        return total

    density_back = [outward(inward(got) * win) for got, win in zip(density_got, windows)]
    photon_back = [
        outward(crosswise(blocks) * win) for blocks, win in zip(photon_parts, windows)
    ]

    def backward(got):
        total = None
        for part, waves in zip(got, tables):
            term = product("ka,zk->az", part.reshape(-1, area), waves)
            total = term if total is None else total + term
        return total

    density_smooth = backward(density_back)
    photon_smooth = backward(photon_back)

    fraction = jnp.clip(photon_smooth / jnp.maximum(density_smooth, 0.5), 0.0, 1.0)
    return fraction.reshape(rows_y, rows_x, grid).transpose(1, 0, 2)


def solution(mesh):
    placed = (
        P(("px", "py"), None),
        P(("px", "py"), None),
        P(("px", "py")),
        P(("px", "py"), None),
        P("px", "py", None),
    )

    return jax.shard_map(
        on_device, mesh=mesh, in_specs=placed, out_specs=P("px", "py", None), check_vma=False
    )
```

```python
import jax
import jax.numpy as jnp
import numpy as np
from jax import lax
from jax.experimental import pallas as pl
from jax.experimental.pallas import tpu as pltpu
from jax.sharding import PartitionSpec as P

RADIUS = 20
LANES = 128
UNROLL = 8
TAB_BITS = 10
SUBLANES = 8


def product(form, left, right):
    return jnp.einsum(form, left, right, precision=lax.Precision.HIGH)


def hartley(length):
    index_row = np.arange(length)
    angle = (index_row[:, None] * index_row[None, :] % length) * (2.0 * np.pi / length)
    return ((np.cos(angle) + np.sin(angle)) / np.sqrt(length)).astype(np.float32)


def sine_cosine(angle):
    turns = jnp.round(angle * np.float32(2.0 / np.pi))
    rest = angle - turns * np.float32(1.5703125)
    rest = rest - turns * np.float32(4.837512969970703e-4)
    rest = rest - turns * np.float32(7.549789948768648e-8)
    square = rest * rest
    sine = ((-1.9515295891e-4 * square + 8.3321608736e-3) * square - 1.6666654611e-1) * (
        square * rest
    ) + rest
    cosine = (
        (2.443315711809948e-5 * square - 1.388731625493765e-3) * square + 4.166664568298827e-2
    ) * (square * square) + (1.0 - 0.5 * square)
    quarter = turns.astype(jnp.int32)
    swap = (quarter & 1) == 1
    first, second = jnp.where(swap, cosine, sine), jnp.where(swap, sine, cosine)
    first = jnp.where((quarter & 2) == 2, -first, first)
    second = jnp.where(((quarter + 1) & 2) == 2, -second, second)
    return first, second


def top_hat(freq_x, freq_y, freq_z, grid):
    radial = jnp.sqrt(freq_x * freq_x + freq_y * freq_y + freq_z * freq_z) * (
        2.0 * jnp.pi * RADIUS / grid
    )
    safe = jnp.where(radial > 0, radial, 1.0)
    sine, cosine = sine_cosine(safe)
    value = 3.0 * (sine - safe * cosine) / (safe * safe * safe)
    return jnp.where(radial > 0, value, 1.0)


def paint_kernel(key, weight, count, waves, out, other):
    rows = out.shape[0]
    step = 256
    sums = (out, other)

    @pl.loop(0, rows // step)
    def _(index):
        part = pl.ds(pl.multiple_of(index * step, step), step)
        for total in sums:
            total[part, :] = jnp.zeros((step, LANES), jnp.float32)

    @pl.loop(0, key.shape[0])
    def _(block):
        turns = lax.div(count[block] + (UNROLL - 1), UNROLL)

        @pl.loop(0, turns)
        def _(turn):
            for lane in range(UNROLL):
                slot = turn * UNROLL + lane
                both = key[block, slot]
                row = pl.ds(lax.shift_right_logical(both, TAB_BITS), 1)
                wave = pl.ds(lax.bitwise_and(both, (1 << TAB_BITS) - 1), 1)
                total = sums[lane % len(sums)]
                total[row, :] = total[row, :] + weight[block, slot] * waves[wave, :]

    @pl.loop(0, rows // step)
    def _(index):
        part = pl.ds(pl.multiple_of(index * step, step), step)
        out[part, :] = out[part, :] + other[part, :]


def paint(key, weight, count, waves, rows):
    smem = pl.BlockSpec(memory_space=pltpu.SMEM)
    vmem = pl.BlockSpec(memory_space=pltpu.VMEM)
    return pl.pallas_call(
        paint_kernel,
        out_shape=jax.ShapeDtypeStruct((rows, LANES), jnp.float32),
        in_specs=[smem, smem, smem, vmem],
        out_specs=vmem,
        scratch_shapes=[pltpu.VMEM((rows, LANES), jnp.float32)],
        cost_estimate=pl.CostEstimate(
            flops=80_000_000_000, bytes_accessed=rows * LANES * 4, transcendentals=0
        ),
        compiler_params=pltpu.CompilerParams(vmem_limit_bytes=3 * rows * LANES * 4),
        name="paint",
    )(key, weight, count, waves)


def halves(values):
    high = values.astype(jnp.bfloat16)
    return high, (values - high.astype(jnp.float32)).astype(jnp.bfloat16)


def split_table(values):
    high = values.astype(jnp.bfloat16)
    return high, (values - np.asarray(high, np.float32)).astype(jnp.bfloat16)


def thrice(left, right, contract):
    form = ((contract, contract), ((), ()))
    (high_l, low_l), (high_r, low_r) = left, right

    def once(one, other):
        return lax.dot_general(one, other, form, preferred_element_type=jnp.float32)

    return once(high_l, high_r) + (once(high_l, low_r) + once(low_l, high_r))


def spread_kernel(high, low, density, out, rows):
    rows_x, deep, grid = density.shape
    tiles = rows_x * deep // LANES
    count = high.shape[0]
    stride = out.shape[0] // count
    flat = density[...].reshape(rows_x * deep, grid)
    for tile in range(grid // LANES):
        rows[tile] = flat[:, tile * LANES : (tile + 1) * LANES]
    lines = jnp.concatenate(
        [
            jnp.concatenate(
                [rows[tile, pl.ds(y, rows_x, stride=deep), :] for y in range(deep)]
            )
            for tile in range(grid // LANES)
        ],
        axis=1,
    )
    spec = thrice((high[...], low[...]), halves(lines), (1,))
    for tile in range(tiles):
        spot = pl.program_id(0) * tiles + tile
        out[pl.ds(spot, count, stride=stride), :] = spec[:, tile * LANES : (tile + 1) * LANES]


def spread(density, waves):
    rows_x, rows_y, grid = density.shape
    high, low = split_table(np.ascontiguousarray(waves.T))
    count = high.shape[0]
    return pl.pallas_call(
        spread_kernel,
        grid=(rows_y // SUBLANES,),
        out_shape=jax.ShapeDtypeStruct((count * rows_x * rows_y // LANES, LANES), jnp.float32),
        in_specs=[
            pl.BlockSpec((count, grid), lambda i: (0, 0)),
            pl.BlockSpec((count, grid), lambda i: (0, 0)),
            pl.BlockSpec((rows_x, SUBLANES, grid), lambda i: (0, i, 0)),
        ],
        out_specs=pl.BlockSpec((count * rows_x * rows_y // LANES, LANES), lambda i: (0, 0)),
        scratch_shapes=[pltpu.VMEM((grid // LANES, rows_x * SUBLANES, LANES), jnp.float32)],
        cost_estimate=pl.CostEstimate(
            flops=6 * count * grid * rows_x * rows_y,
            bytes_accessed=4 * rows_x * rows_y * (grid + count),
            transcendentals=0,
        ),
        compiler_params=pltpu.CompilerParams(vmem_limit_bytes=40 << 20),
        name="spread",
    )(jnp.asarray(high), jnp.asarray(low), density)


def finish_kernel(high, low, last, photon, density, out, rows):
    rows_x, deep, grid = out.shape
    tiles = rows_x * deep // LANES
    count = high.shape[0]
    stride = last.shape[0] // count
    spec = jnp.concatenate(
        [
            last[pl.ds(pl.program_id(0) * tiles + tile, count, stride=stride), :]
            for tile in range(tiles)
        ],
        axis=1,
    )
    field = thrice(halves(spec), (high[...], low[...]), (0,)) + photon[...]
    fraction = jnp.clip(field / jnp.maximum(density[...], 0.5), 0.0, 1.0)
    for tile in range(grid // LANES):
        lanes = slice(tile * LANES, (tile + 1) * LANES)
        for y in range(deep):
            rows[tile, pl.ds(y, rows_x, stride=deep), :] = fraction[
                y * rows_x : (y + 1) * rows_x, lanes
            ]
        out[:, :, lanes] = rows[tile].reshape(rows_x, deep, LANES)


def finish(last, photon, density, waves, rows_x, rows_y):
    grid = photon.shape[1]
    high, low = split_table(np.ascontiguousarray(waves.T))
    count = high.shape[0]
    last = last.reshape(-1, LANES)
    share = rows_x * SUBLANES
    return pl.pallas_call(
        finish_kernel,
        grid=(rows_y // SUBLANES,),
        out_shape=jax.ShapeDtypeStruct((rows_x, rows_y, grid), jnp.float32),
        in_specs=[
            pl.BlockSpec((count, grid), lambda i: (0, 0)),
            pl.BlockSpec((count, grid), lambda i: (0, 0)),
            pl.BlockSpec(last.shape, lambda i: (0, 0)),
            pl.BlockSpec((share, grid), lambda i: (i, 0)),
            pl.BlockSpec((share, grid), lambda i: (i, 0)),
        ],
        out_specs=pl.BlockSpec((rows_x, SUBLANES, grid), lambda i: (0, i, 0)),
        scratch_shapes=[pltpu.VMEM((grid // LANES, share, LANES), jnp.float32)],
        cost_estimate=pl.CostEstimate(
            flops=6 * count * grid * rows_x * rows_y,
            bytes_accessed=4 * rows_x * rows_y * (3 * grid + count),
            transcendentals=0,
        ),
        compiler_params=pltpu.CompilerParams(vmem_limit_bytes=40 << 20),
        name="finish",
    )(jnp.asarray(high), jnp.asarray(low), last, photon, density)


def gather_kernel(mine, everyone, send_sems, receive_sems):
    count = everyone.shape[0]
    me = lax.axis_index("py")
    barrier = pltpu.get_barrier_semaphore()
    for shift in range(1, count):
        pl.semaphore_signal(
            barrier, inc=1, device_id={"py": lax.rem(me + shift, count)},
            device_id_type=pl.DeviceIdType.MESH,
        )
    pl.semaphore_wait(barrier, count - 1)
    copies = [
        pltpu.make_async_remote_copy(
            mine, everyone.at[me], send_sems.at[shift], receive_sems.at[shift],
            device_id={"py": lax.rem(me + shift, count)},
            device_id_type=pl.DeviceIdType.MESH,
        )
        for shift in range(1, count)
    ]
    for copy in copies:
        copy.start()
    everyone[pl.ds(me, 1)] = mine[...][None]
    for copy in copies:
        copy.wait()


def gather(mine, count):
    vmem = pl.BlockSpec(memory_space=pltpu.VMEM)
    return pl.pallas_call(
        gather_kernel,
        out_shape=jax.ShapeDtypeStruct((count,) + mine.shape, mine.dtype),
        in_specs=[vmem],
        out_specs=vmem,
        scratch_shapes=[pltpu.SemaphoreType.DMA((count,)), pltpu.SemaphoreType.DMA((count,))],
        compiler_params=pltpu.CompilerParams(collective_id=0, has_side_effects=True),
        name="gather",
    )(mine)


def on_device(photons, halo_cells, halo_counts, owners, density):
    rows_x, rows_y, grid = density.shape
    slots = photons.shape[1]
    count_x = lax.axis_size("px")
    count_y = lax.axis_size("py")
    place_x = lax.axis_index("px")
    place_y = lax.axis_index("py")
    devices_all = count_x * count_y
    planes = grid // devices_all
    area = rows_x * rows_y
    table_np = hartley(grid)
    table = jnp.asarray(table_np)
    table_x = table.reshape(count_x, rows_x, grid)
    table_y = table.reshape(count_y, rows_y, grid)

    first = max(1, planes * 2 // 3)
    assert first < planes
    parts = [(0, first), (first, planes)]
    by_plane = table_np.reshape(grid, devices_all, planes)
    tables = [by_plane[:, :, a:b].reshape(grid, devices_all * (b - a)) for a, b in parts]

    pair = LANES // 2
    width = pair // count_x
    assert planes <= width and rows_x % 2 == 0
    assert 2 * grid <= 1 << TAB_BITS and rows_x * grid * grid < 1 << 24
    half_x = rows_x // 2
    rows = grid * half_x
    slot_index = jnp.arange(slots, dtype=jnp.int32)[None, :]
    live = slot_index < halo_counts[:, None]
    weights = jnp.where(live, photons, 0.0)
    cell_x = halo_cells // (rows_y * grid)
    cell_y = owners * rows_y + halo_cells // grid % rows_y
    cell_z = halo_cells % grid
    row = (cell_x // 2) * grid + cell_y
    key = jnp.where(live, row * (2 * grid) + (cell_x % 2) * grid + cell_z, 0)
    sent = jnp.concatenate([weights, key.astype(jnp.float32)])
    slab = gather(sent, count_y).reshape(count_y, 2, -1, slots)
    slab = [slab[:, kind].reshape(-1, slots) for kind in range(2)]
    slab, density = lax.optimization_barrier((slab, density))

    def signed(index_values):
        return jnp.where(index_values < grid // 2, index_values, index_values - grid).astype(
            jnp.float32
        )

    received = []

    def exchange(blocks_out):
        blocks_out = blocks_out.reshape(devices_all, -1, LANES)
        if received:
            blocks_out, _ = lax.optimization_barrier((blocks_out, received[-1]))
        got = lax.all_to_all(
            blocks_out, ("px", "py"), split_axis=0, concat_axis=0, tiled=True
        )
        received.append(got)
        return got

    specs = [spread(density, part) for part in tables]
    density_got = [exchange(specs[0])]

    freq = signed(jnp.arange(grid, dtype=jnp.int32))
    freq_z = signed(
        lax.axis_index(("px", "py")) * planes + jnp.arange(planes, dtype=jnp.int32)
    )
    windows = [
        lax.optimization_barrier(
            top_hat(freq_z[a:b, None, None], freq[None, :, None], freq[None, None, :], grid)
        )
        for a, b in parts
    ]

    all_keys = slab[1].astype(jnp.int32)
    all_keys = all_keys // (2 * grid) * (1 << TAB_BITS) + all_keys % (2 * grid)
    all_counts = jnp.max(jnp.where(slab[0] != 0.0, slot_index + 1, 0), axis=1)
    own = lax.dynamic_index_in_dim(
        table.reshape(grid, count_x, count_y, planes), place_y, 2, keepdims=False
    )
    own = jnp.pad(own, ((0, 0), (0, 0), (0, width - planes))).reshape(grid, pair)
    waves = jnp.concatenate(
        [jnp.pad(own, ((0, 0), (0, pair))), jnp.pad(own, ((0, 0), (pair, 0)))]
    )
    painted = paint(all_keys, slab[0], all_counts, waves, rows)
    for spec in specs[1:]:
        spec, painted, windows[0] = lax.optimization_barrier((spec, painted, windows[0]))
        density_got.append(exchange(spec))

    def outward(full):
        half = product("kmn,qlm->qkln", full, table_y)
        back = product("qkln,ixn->iqklx", half, table_x)
        return exchange(back)

    def inward(got):
        got = got.reshape(count_x, count_y, -1, rows_y, rows_x)
        half = product("iqklx,ixn->qkln", got, table_x)
        return product("qkln,qlm->kmn", half, table_y)

    lines = product("ayc,ym->acm", painted.reshape(half_x, grid, LANES), table)
    lines = lines.reshape(rows_x, count_x, width, grid)[:, :, :planes]
    lines = lines.transpose(1, 2, 0, 3)
    rows_of = [
        lax.dynamic_index_in_dim(table_x, (place_x - shift) % count_x, 0, keepdims=False)
        for shift in range(count_x)
    ]
    photon_parts = [
        [
            lax.dynamic_slice(
                lines, ((place_x + shift) % count_x, a, 0, 0), (1, b - a, rows_x, grid)
            )[0]
            for shift in range(count_x)
        ]
        for a, b in parts
    ]

    def around(block, shift):
        if shift == 0:
            return block
        return lax.ppermute(block, "px", [(i, (i + shift) % count_x) for i in range(count_x)])

    photon_parts = [
        [around(block, shift) for shift, block in enumerate(blocks)]
        for blocks in photon_parts
    ]

    def crosswise(blocks):
        total = None
        for block, rows_from in zip(blocks, rows_of):
            term = product("kxm,xn->kmn", block, rows_from)
            total = term if total is None else total + term
        return total

    density_back = [outward(inward(got) * win) for got, win in zip(density_got, windows)]
    photon_back = [
        outward(crosswise(blocks) * win) for blocks, win in zip(photon_parts, windows)
    ]

    def backward(got):
        total = None
        for part, waves in zip(got, tables):
            term = product("ka,zk->az", part.reshape(-1, area), jnp.asarray(waves))
            total = term if total is None else total + term
        return total

    density_smooth = backward(density_back)
    photon_smooth = backward(photon_back[:-1])
    return finish(
        photon_back[-1], photon_smooth, density_smooth, tables[-1], rows_x, rows_y
    )


def solution(mesh):
    placed = (
        P(("px", "py"), None),
        P(("px", "py"), None),
        P(("px", "py")),
        P(("px", "py"), None),
        P("px", "py", None),
    )

    return jax.shard_map(
        on_device, mesh=mesh, in_specs=placed, out_specs=P("px", "py", None), check_vma=False
    )
```

```python
import functools

import jax
import jax.numpy as jnp
import numpy as np
from jax import lax
from jax.experimental import pallas as pl
from jax.experimental.pallas import tpu as pltpu
from jax.sharding import PartitionSpec as P

RADIUS = 20
LANES = 128
UNROLL = 8
TAB_BITS = 10
SUBLANES = 8


def product(form, left, right):
    return jnp.einsum(form, left, right, precision=lax.Precision.HIGH)


def hartley(length):
    index_row = np.arange(length)
    angle = (index_row[:, None] * index_row[None, :] % length) * (2.0 * np.pi / length)
    return ((np.cos(angle) + np.sin(angle)) / np.sqrt(length)).astype(np.float32)


def sine_cosine(angle):
    turns = jnp.round(angle * np.float32(2.0 / np.pi))
    rest = angle - turns * np.float32(1.5703125)
    rest = rest - turns * np.float32(4.837512969970703e-4)
    rest = rest - turns * np.float32(7.549789948768648e-8)
    square = rest * rest
    sine = ((-1.9515295891e-4 * square + 8.3321608736e-3) * square - 1.6666654611e-1) * (
        square * rest
    ) + rest
    cosine = (
        (2.443315711809948e-5 * square - 1.388731625493765e-3) * square + 4.166664568298827e-2
    ) * (square * square) + (1.0 - 0.5 * square)
    quarter = turns.astype(jnp.int32)
    swap = (quarter & 1) == 1
    first, second = jnp.where(swap, cosine, sine), jnp.where(swap, sine, cosine)
    first = jnp.where((quarter & 2) == 2, -first, first)
    second = jnp.where(((quarter + 1) & 2) == 2, -second, second)
    return first, second


def top_hat(freq_x, freq_y, freq_z, grid):
    radial = jnp.sqrt(freq_x * freq_x + freq_y * freq_y + freq_z * freq_z) * (
        2.0 * jnp.pi * RADIUS / grid
    )
    safe = jnp.where(radial > 0, radial, 1.0)
    sine, cosine = sine_cosine(safe)
    value = 3.0 * (sine - safe * cosine) / (safe * safe * safe)
    return jnp.where(radial > 0, value, 1.0)


def paint_kernel(key, weight, count, waves, out, other):
    rows = out.shape[0]
    step = 256
    sums = (out, other)

    @pl.loop(0, rows // step)
    def _(index):
        part = pl.ds(pl.multiple_of(index * step, step), step)
        for total in sums:
            total[part, :] = jnp.zeros((step, LANES), jnp.float32)

    @pl.loop(0, key.shape[0])
    def _(block):
        turns = lax.div(count[block] + (UNROLL - 1), UNROLL)

        @pl.loop(0, turns)
        def _(turn):
            for lane in range(UNROLL):
                slot = turn * UNROLL + lane
                both = key[block, slot]
                row = pl.ds(lax.shift_right_logical(both, TAB_BITS), 1)
                wave = pl.ds(lax.bitwise_and(both, (1 << TAB_BITS) - 1), 1)
                total = sums[lane % len(sums)]
                total[row, :] = total[row, :] + weight[block, slot] * waves[wave, :]

    @pl.loop(0, rows // step)
    def _(index):
        part = pl.ds(pl.multiple_of(index * step, step), step)
        out[part, :] = out[part, :] + other[part, :]


def paint(key, weight, count, waves, rows):
    smem = pl.BlockSpec(memory_space=pltpu.SMEM)
    vmem = pl.BlockSpec(memory_space=pltpu.VMEM)
    return pl.pallas_call(
        paint_kernel,
        out_shape=jax.ShapeDtypeStruct((rows, LANES), jnp.float32),
        in_specs=[smem, smem, smem, vmem],
        out_specs=vmem,
        scratch_shapes=[pltpu.VMEM((rows, LANES), jnp.float32)],
        cost_estimate=pl.CostEstimate(
            flops=80_000_000_000, bytes_accessed=rows * LANES * 4, transcendentals=0
        ),
        compiler_params=pltpu.CompilerParams(vmem_limit_bytes=3 * rows * LANES * 4),
        name="paint",
    )(key, weight, count, waves)


def halves(values):
    high = values.astype(jnp.bfloat16)
    return high, (values - high.astype(jnp.float32)).astype(jnp.bfloat16)


def split_table(values):
    high = values.astype(jnp.bfloat16)
    return high, (values - np.asarray(high, np.float32)).astype(jnp.bfloat16)


def thrice(left, right, contract):
    form = ((contract, contract), ((), ()))
    (high_l, low_l), (high_r, low_r) = left, right

    def once(one, other):
        return lax.dot_general(one, other, form, preferred_element_type=jnp.float32)

    return once(high_l, high_r) + (once(high_l, low_r) + once(low_l, high_r))


def spread_kernel(high, low, density, out, rows):
    rows_x, deep, grid = density.shape
    tiles = rows_x * deep // LANES
    count = high.shape[0]
    stride = out.shape[0] // count
    flat = density[...].reshape(rows_x * deep, grid)
    for tile in range(grid // LANES):
        rows[tile] = flat[:, tile * LANES : (tile + 1) * LANES]
    lines = jnp.concatenate(
        [
            jnp.concatenate(
                [rows[tile, pl.ds(y, rows_x, stride=deep), :] for y in range(deep)]
            )
            for tile in range(grid // LANES)
        ],
        axis=1,
    )
    spec = thrice((high[...], low[...]), halves(lines), (1,))
    for tile in range(tiles):
        spot = pl.program_id(0) * tiles + tile
        out[pl.ds(spot, count, stride=stride), :] = spec[:, tile * LANES : (tile + 1) * LANES]


def spread(density, waves):
    rows_x, rows_y, grid = density.shape
    high, low = split_table(np.ascontiguousarray(waves.T))
    count = high.shape[0]
    return pl.pallas_call(
        spread_kernel,
        grid=(rows_y // SUBLANES,),
        out_shape=jax.ShapeDtypeStruct((count * rows_x * rows_y // LANES, LANES), jnp.float32),
        in_specs=[
            pl.BlockSpec((count, grid), lambda i: (0, 0)),
            pl.BlockSpec((count, grid), lambda i: (0, 0)),
            pl.BlockSpec((rows_x, SUBLANES, grid), lambda i: (0, i, 0)),
        ],
        out_specs=pl.BlockSpec((count * rows_x * rows_y // LANES, LANES), lambda i: (0, 0)),
        scratch_shapes=[pltpu.VMEM((grid // LANES, rows_x * SUBLANES, LANES), jnp.float32)],
        cost_estimate=pl.CostEstimate(
            flops=6 * count * grid * rows_x * rows_y,
            bytes_accessed=4 * rows_x * rows_y * (grid + count),
            transcendentals=0,
        ),
        compiler_params=pltpu.CompilerParams(vmem_limit_bytes=40 << 20),
        name="spread",
    )(jnp.asarray(high), jnp.asarray(low), density)


def finish_kernel(high, low, last, photon, density, out, rows):
    rows_x, deep, grid = out.shape
    tiles = rows_x * deep // LANES
    count = high.shape[0]
    stride = last.shape[0] // count
    spec = jnp.concatenate(
        [
            last[pl.ds(pl.program_id(0) * tiles + tile, count, stride=stride), :]
            for tile in range(tiles)
        ],
        axis=1,
    )
    field = thrice(halves(spec), (high[...], low[...]), (0,)) + photon[...]
    fraction = jnp.clip(field / jnp.maximum(density[...], 0.5), 0.0, 1.0)
    for tile in range(grid // LANES):
        lanes = slice(tile * LANES, (tile + 1) * LANES)
        for y in range(deep):
            rows[tile, pl.ds(y, rows_x, stride=deep), :] = fraction[
                y * rows_x : (y + 1) * rows_x, lanes
            ]
        out[:, :, lanes] = rows[tile].reshape(rows_x, deep, LANES)


def finish(last, photon, density, waves, rows_x, rows_y):
    grid = photon.shape[1]
    high, low = split_table(np.ascontiguousarray(waves.T))
    count = high.shape[0]
    last = last.reshape(-1, LANES)
    share = rows_x * SUBLANES
    return pl.pallas_call(
        finish_kernel,
        grid=(rows_y // SUBLANES,),
        out_shape=jax.ShapeDtypeStruct((rows_x, rows_y, grid), jnp.float32),
        in_specs=[
            pl.BlockSpec((count, grid), lambda i: (0, 0)),
            pl.BlockSpec((count, grid), lambda i: (0, 0)),
            pl.BlockSpec(last.shape, lambda i: (0, 0)),
            pl.BlockSpec((share, grid), lambda i: (i, 0)),
            pl.BlockSpec((share, grid), lambda i: (i, 0)),
        ],
        out_specs=pl.BlockSpec((rows_x, SUBLANES, grid), lambda i: (0, i, 0)),
        scratch_shapes=[pltpu.VMEM((grid // LANES, share, LANES), jnp.float32)],
        cost_estimate=pl.CostEstimate(
            flops=6 * count * grid * rows_x * rows_y,
            bytes_accessed=4 * rows_x * rows_y * (3 * grid + count),
            transcendentals=0,
        ),
        compiler_params=pltpu.CompilerParams(vmem_limit_bytes=40 << 20),
        name="finish",
    )(jnp.asarray(high), jnp.asarray(low), last, photon, density)


def gather_kernel(inner, mine, everyone, send_sems, receive_sems):
    count = everyone.shape[0]
    me = lax.axis_index("ph") * inner + lax.axis_index("pl")

    def peer(shift):
        other = lax.rem(me + shift, count)
        return {"ph": lax.div(other, inner), "pl": lax.rem(other, inner)}

    barrier = pltpu.get_barrier_semaphore()
    for shift in range(1, count):
        pl.semaphore_signal(
            barrier, inc=1, device_id=peer(shift),
            device_id_type=pl.DeviceIdType.MESH,
        )
    pl.semaphore_wait(barrier, count - 1)
    copies = [
        pltpu.make_async_remote_copy(
            mine, everyone.at[me], send_sems.at[shift], receive_sems.at[shift],
            device_id=peer(shift),
            device_id_type=pl.DeviceIdType.MESH,
        )
        for shift in range(1, count)
    ]
    for copy in copies:
        copy.start()
    everyone[pl.ds(me, 1)] = mine[...][None]
    for copy in copies:
        copy.wait()


def gather(mine, count, inner):
    vmem = pl.BlockSpec(memory_space=pltpu.VMEM)
    return pl.pallas_call(
        functools.partial(gather_kernel, inner),
        out_shape=jax.ShapeDtypeStruct((count,) + mine.shape, mine.dtype),
        in_specs=[vmem],
        out_specs=vmem,
        scratch_shapes=[pltpu.SemaphoreType.DMA((count,)), pltpu.SemaphoreType.DMA((count,))],
        compiler_params=pltpu.CompilerParams(collective_id=0, has_side_effects=True),
        name="gather",
    )(mine)


def on_device(photons, halo_cells, halo_counts, owners, density):
    rows_x, rows_y, grid = density.shape
    slots = photons.shape[1]
    count_x = lax.axis_size("px")
    count_h, count_l = lax.axis_size("ph"), lax.axis_size("pl")
    count_y = count_h * count_l
    place_x, place_h, place_l = (lax.axis_index(name) for name in ("px", "ph", "pl"))
    place_y = place_h * count_l + place_l
    devices_all = count_x * count_y
    planes = grid // devices_all
    area = rows_x * rows_y
    table_np = hartley(grid)
    table = jnp.asarray(table_np)
    table_x = table.reshape(count_x, rows_x, grid)
    table_y = table.reshape(count_y, rows_y, grid)

    first = max(1, planes * 2 // 3)
    assert first < planes
    parts = [(0, first), (first, planes)]
    shared = np.arange(grid).reshape(count_x, count_h, count_l, planes)[..., first:]
    shared = shared.transpose(0, 2, 1, 3).reshape(count_x, count_l, -1)
    by_plane = table_np.reshape(grid, devices_all, planes)
    tables = [by_plane[:, :, a:b].reshape(grid, devices_all * (b - a)) for a, b in parts]

    pair = LANES // 2
    width = pair // count_x
    assert rows_x % 2 == 0
    assert 2 * grid <= 1 << TAB_BITS and rows_x * grid * grid < 1 << 24
    half_x = rows_x // 2
    rows = grid * half_x
    slot_index = jnp.arange(slots, dtype=jnp.int32)[None, :]
    live = slot_index < halo_counts[:, None]
    weights = jnp.where(live, photons, 0.0)
    cell_x = halo_cells // (rows_y * grid)
    cell_y = owners * rows_y + halo_cells // grid % rows_y
    cell_z = halo_cells % grid
    row = (cell_x // 2) * grid + cell_y
    key = jnp.where(live, row * (2 * grid) + (cell_x % 2) * grid + cell_z, 0)
    sent = jnp.concatenate([weights, key.astype(jnp.float32)])
    slab = gather(sent, count_y, count_l).reshape(count_y, 2, -1, slots)
    slab = [slab[:, kind].reshape(-1, slots) for kind in range(2)]
    slab, density = lax.optimization_barrier((slab, density))

    def signed(index_values):
        return jnp.where(index_values < grid // 2, index_values, index_values - grid).astype(
            jnp.float32
        )

    received = []

    def exchange(blocks_out, among=("px", "ph", "pl")):
        blocks_out = blocks_out.reshape(lax.axis_size(among), -1, LANES)
        if received:
            blocks_out, _ = lax.optimization_barrier((blocks_out, received[-1]))
        got = lax.all_to_all(
            blocks_out, among, split_axis=0, concat_axis=0, tiled=True
        )
        received.append(got)
        return got

    specs = [spread(density, part) for part in tables]
    density_got = [exchange(specs[0])]

    freq = signed(jnp.arange(grid, dtype=jnp.int32))
    freq_z = signed(
        (place_x * count_y + place_y) * planes + jnp.arange(planes, dtype=jnp.int32)
    )
    shared_z = signed(jnp.asarray(shared, dtype=jnp.int32)[place_x, place_l])

    def window_of(freq_z):
        return lax.optimization_barrier(
            top_hat(freq_z[:, None, None], freq[None, :, None], freq[None, None, :], grid)
        )

    rest = window_of(jnp.concatenate([freq_z[first:], shared_z]))
    windows = [window_of(freq_z[:first]), rest[: planes - first]]
    shared_window = rest[planes - first :]

    all_keys = slab[1].astype(jnp.int32)
    all_keys = all_keys // (2 * grid) * (1 << TAB_BITS) + all_keys % (2 * grid)
    all_counts = jnp.max(jnp.where(slab[0] != 0.0, slot_index + 1, 0), axis=1)
    alone = np.arange(grid).reshape(count_x, count_y, planes)[..., :first]
    columns = np.concatenate(
        [
            alone.transpose(1, 0, 2),
            np.tile(shared.transpose(1, 0, 2), (count_h, 1, 1)),
        ],
        axis=2,
    )
    used = columns.shape[2]
    assert used <= width
    own = np.zeros((count_y, grid, count_x, width), np.float32)
    own[..., :used] = table_np[:, columns].transpose(1, 0, 2, 3)
    own = jnp.asarray(own.reshape(count_y, grid, pair))[place_y]
    waves = jnp.concatenate(
        [jnp.pad(own, ((0, 0), (0, pair))), jnp.pad(own, ((0, 0), (pair, 0)))]
    )
    painted = paint(all_keys, slab[0], all_counts, waves, rows)
    for spec in specs[1:]:
        spec, painted = lax.optimization_barrier((spec, painted))
        density_got.append(exchange(spec))

    half_y = lax.dynamic_index_in_dim(
        table_y.reshape(count_h, count_l, rows_y, grid), place_h, 0, keepdims=False
    )

    def outward(full, sums_y=table_y, among=("px", "ph", "pl")):
        half = product("kmn,qlm->qkln", full, sums_y)
        back = product("qkln,ixn->iqklx", half, table_x)
        return exchange(back, among)

    def inward(got):
        got = got.reshape(count_x, count_y, -1, rows_y, rows_x)
        half = product("iqklx,ixn->qkln", got, table_x)
        return product("qkln,qlm->kmn", half, table_y)

    lines = product("ayc,ym->acm", painted.reshape(half_x, grid, LANES), table)
    lines = lines.reshape(rows_x, count_x, width, grid)[:, :, :used]
    lines = lines.transpose(1, 2, 0, 3)
    rows_of = [
        lax.dynamic_index_in_dim(table_x, (place_x - shift) % count_x, 0, keepdims=False)
        for shift in range(count_x)
    ]
    photon_parts = [
        [
            lax.dynamic_slice(
                lines, ((place_x + shift) % count_x, a, 0, 0), (1, b - a, rows_x, grid)
            )[0]
            for shift in range(count_x)
        ]
        for a, b in ((0, first), (first, used))
    ]

    def around(block, shift):
        if shift == 0:
            return block
        return lax.ppermute(block, "px", [(i, (i + shift) % count_x) for i in range(count_x)])

    photon_parts = [
        [around(block, shift) for shift, block in enumerate(blocks)]
        for blocks in photon_parts
    ]

    def crosswise(blocks):
        total = None
        for block, rows_from in zip(blocks, rows_of):
            term = product("kxm,xn->kmn", block, rows_from)
            total = term if total is None else total + term
        return total

    density_back = [outward(inward(got) * win) for got, win in zip(density_got, windows)]
    across = crosswise(photon_parts[0])
    photon_first = outward(across * windows[0])
    photon_last = outward(
        crosswise(photon_parts[1]) * shared_window, half_y, ("px", "pl")
    )

    def backward(got):
        total = None
        for part, waves in zip(got, tables):
            term = product("ka,zk->az", part.reshape(-1, area), jnp.asarray(waves))
            total = term if total is None else total + term
        return total

    density_smooth = backward(density_back)
    photon_smooth = backward([photon_first])
    return finish(
        photon_last, photon_smooth, density_smooth, table_np[:, shared.reshape(-1)], rows_x, rows_y
    )


def solution(mesh):
    devices = mesh.devices
    count_x, count_y = devices.shape
    inner = jax.sharding.Mesh(devices.reshape(count_x, 2, count_y // 2), ("px", "ph", "pl"))
    every, split = ("px", "ph", "pl"), ("ph", "pl")
    placed = (P(every, None), P(every, None), P(every), P(every, None), P("px", split, None))

    return jax.shard_map(
        on_device, mesh=inner, in_specs=placed, out_specs=P("px", split, None), check_vma=False
    )
```

```python
import functools

import jax
import jax.numpy as jnp
import numpy as np
from jax import lax
from jax.experimental import pallas as pl
from jax.experimental.pallas import tpu as pltpu
from jax.sharding import PartitionSpec as P

RADIUS = 20
LANES = 128
UNROLL = 8
TAB_BITS = 10
SUBLANES = 8


def product(form, left, right):
    return jnp.einsum(form, left, right, precision=lax.Precision.HIGH)


def hartley(length):
    index_row = np.arange(length)
    angle = (index_row[:, None] * index_row[None, :] % length) * (2.0 * np.pi / length)
    return ((np.cos(angle) + np.sin(angle)) / np.sqrt(length)).astype(np.float32)


def sine_cosine(angle):
    turns = jnp.round(angle * np.float32(2.0 / np.pi))
    rest = angle - turns * np.float32(1.5703125)
    rest = rest - turns * np.float32(4.837512969970703e-4)
    rest = rest - turns * np.float32(7.549789948768648e-8)
    square = rest * rest
    sine = ((-1.9515295891e-4 * square + 8.3321608736e-3) * square - 1.6666654611e-1) * (
        square * rest
    ) + rest
    cosine = (
        (2.443315711809948e-5 * square - 1.388731625493765e-3) * square + 4.166664568298827e-2
    ) * (square * square) + (1.0 - 0.5 * square)
    quarter = turns.astype(jnp.int32)
    swap = (quarter & 1) == 1
    first, second = jnp.where(swap, cosine, sine), jnp.where(swap, sine, cosine)
    first = jnp.where((quarter & 2) == 2, -first, first)
    second = jnp.where(((quarter + 1) & 2) == 2, -second, second)
    return first, second


def top_hat(freq_x, freq_y, freq_z, grid):
    radial = jnp.sqrt(freq_x * freq_x + freq_y * freq_y + freq_z * freq_z) * (
        2.0 * jnp.pi * RADIUS / grid
    )
    safe = jnp.where(radial > 0, radial, 1.0)
    sine, cosine = sine_cosine(safe)
    value = 3.0 * (sine - safe * cosine) / (safe * safe * safe)
    return jnp.where(radial > 0, value, 1.0)


def paint_kernel(key, weight, count, waves, out, other):
    rows = out.shape[0]
    step = 256
    sums = (out, other)

    @pl.loop(0, rows // step)
    def _(index):
        part = pl.ds(pl.multiple_of(index * step, step), step)
        for total in sums:
            total[part, :] = jnp.zeros((step, LANES), jnp.float32)

    @pl.loop(0, key.shape[0])
    def _(block):
        turns = lax.div(count[block] + (UNROLL - 1), UNROLL)

        @pl.loop(0, turns)
        def _(turn):
            for lane in range(UNROLL):
                slot = turn * UNROLL + lane
                both = key[block, slot]
                row = pl.ds(lax.shift_right_logical(both, TAB_BITS), 1)
                wave = pl.ds(lax.bitwise_and(both, (1 << TAB_BITS) - 1), 1)
                total = sums[lane % len(sums)]
                total[row, :] = total[row, :] + weight[block, slot] * waves[wave, :]

    @pl.loop(0, rows // step)
    def _(index):
        part = pl.ds(pl.multiple_of(index * step, step), step)
        out[part, :] = out[part, :] + other[part, :]


def paint(key, weight, count, waves, rows):
    smem = pl.BlockSpec(memory_space=pltpu.SMEM)
    vmem = pl.BlockSpec(memory_space=pltpu.VMEM)
    return pl.pallas_call(
        paint_kernel,
        out_shape=jax.ShapeDtypeStruct((rows, LANES), jnp.float32),
        in_specs=[smem, smem, smem, vmem],
        out_specs=vmem,
        scratch_shapes=[pltpu.VMEM((rows, LANES), jnp.float32)],
        cost_estimate=pl.CostEstimate(
            flops=80_000_000_000, bytes_accessed=rows * LANES * 4, transcendentals=0
        ),
        compiler_params=pltpu.CompilerParams(vmem_limit_bytes=3 * rows * LANES * 4),
        name="paint",
    )(key, weight, count, waves)


def halves(values):
    high = values.astype(jnp.bfloat16)
    return high, (values - high.astype(jnp.float32)).astype(jnp.bfloat16)


def split_table(values):
    high = values.astype(jnp.bfloat16)
    return high, (values - np.asarray(high, np.float32)).astype(jnp.bfloat16)


def thrice(left, right, contract):
    form = ((contract, contract), ((), ()))
    (high_l, low_l), (high_r, low_r) = left, right

    def once(one, other):
        return lax.dot_general(one, other, form, preferred_element_type=jnp.float32)

    return once(high_l, high_r) + (once(high_l, low_r) + once(low_l, high_r))


def spread_kernel(high, low, density, out, rows):
    rows_x, deep, grid = density.shape
    tiles = rows_x * deep // LANES
    count = high.shape[0]
    stride = out.shape[0] // count
    flat = density[...].reshape(rows_x * deep, grid)
    for tile in range(grid // LANES):
        rows[tile] = flat[:, tile * LANES : (tile + 1) * LANES]
    lines = jnp.concatenate(
        [
            jnp.concatenate(
                [rows[tile, pl.ds(y, rows_x, stride=deep), :] for y in range(deep)]
            )
            for tile in range(grid // LANES)
        ],
        axis=1,
    )
    spec = thrice((high[...], low[...]), halves(lines), (1,))
    for tile in range(tiles):
        spot = pl.program_id(0) * tiles + tile
        out[pl.ds(spot, count, stride=stride), :] = spec[:, tile * LANES : (tile + 1) * LANES]


def spread(density, waves):
    rows_x, rows_y, grid = density.shape
    high, low = split_table(np.ascontiguousarray(waves.T))
    count = high.shape[0]
    return pl.pallas_call(
        spread_kernel,
        grid=(rows_y // SUBLANES,),
        out_shape=jax.ShapeDtypeStruct((count * rows_x * rows_y // LANES, LANES), jnp.float32),
        in_specs=[
            pl.BlockSpec((count, grid), lambda i: (0, 0)),
            pl.BlockSpec((count, grid), lambda i: (0, 0)),
            pl.BlockSpec((rows_x, SUBLANES, grid), lambda i: (0, i, 0)),
        ],
        out_specs=pl.BlockSpec((count * rows_x * rows_y // LANES, LANES), lambda i: (0, 0)),
        scratch_shapes=[pltpu.VMEM((grid // LANES, rows_x * SUBLANES, LANES), jnp.float32)],
        cost_estimate=pl.CostEstimate(
            flops=6 * count * grid * rows_x * rows_y,
            bytes_accessed=4 * rows_x * rows_y * (grid + count),
            transcendentals=0,
        ),
        compiler_params=pltpu.CompilerParams(vmem_limit_bytes=62 << 20),
        name="spread",
    )(jnp.asarray(high), jnp.asarray(low), density)


def finish_kernel(high, low, last, photon, density, out, rows):
    rows_x, deep, grid = out.shape
    tiles = rows_x * deep // LANES
    count = high.shape[0]
    stride = last.shape[0] // count
    spec = jnp.concatenate(
        [
            last[pl.ds(pl.program_id(0) * tiles + tile, count, stride=stride), :]
            for tile in range(tiles)
        ],
        axis=1,
    )
    field = thrice(halves(spec), (high[...], low[...]), (0,)) + photon[...]
    fraction = jnp.clip(field / jnp.maximum(density[...], 0.5), 0.0, 1.0)
    for tile in range(grid // LANES):
        lanes = slice(tile * LANES, (tile + 1) * LANES)
        for y in range(deep):
            rows[tile, pl.ds(y, rows_x, stride=deep), :] = fraction[
                y * rows_x : (y + 1) * rows_x, lanes
            ]
        out[:, :, lanes] = rows[tile].reshape(rows_x, deep, LANES)


def finish(last, photon, density, waves, rows_x, rows_y):
    grid = photon.shape[1]
    high, low = split_table(np.ascontiguousarray(waves.T))
    count = high.shape[0]
    last = last.reshape(-1, LANES)
    share = rows_x * SUBLANES
    return pl.pallas_call(
        finish_kernel,
        grid=(rows_y // SUBLANES,),
        out_shape=jax.ShapeDtypeStruct((rows_x, rows_y, grid), jnp.float32),
        in_specs=[
            pl.BlockSpec((count, grid), lambda i: (0, 0)),
            pl.BlockSpec((count, grid), lambda i: (0, 0)),
            pl.BlockSpec(last.shape, lambda i: (0, 0)),
            pl.BlockSpec((share, grid), lambda i: (i, 0)),
            pl.BlockSpec((share, grid), lambda i: (i, 0)),
        ],
        out_specs=pl.BlockSpec((rows_x, SUBLANES, grid), lambda i: (0, i, 0)),
        scratch_shapes=[pltpu.VMEM((grid // LANES, share, LANES), jnp.float32)],
        cost_estimate=pl.CostEstimate(
            flops=6 * count * grid * rows_x * rows_y,
            bytes_accessed=4 * rows_x * rows_y * (3 * grid + count),
            transcendentals=0,
        ),
        compiler_params=pltpu.CompilerParams(vmem_limit_bytes=62 << 20),
        name="finish",
    )(jnp.asarray(high), jnp.asarray(low), last, photon, density)


def gather_kernel(inner, mine, everyone, send_sems, receive_sems):
    count = everyone.shape[0]
    me = lax.axis_index("ph") * inner + lax.axis_index("pl")

    def peer(shift):
        other = lax.rem(me + shift, count)
        return {"ph": lax.div(other, inner), "pl": lax.rem(other, inner)}

    barrier = pltpu.get_barrier_semaphore()
    for shift in range(1, count):
        pl.semaphore_signal(
            barrier, inc=1, device_id=peer(shift),
            device_id_type=pl.DeviceIdType.MESH,
        )
    pl.semaphore_wait(barrier, count - 1)
    copies = [
        pltpu.make_async_remote_copy(
            mine, everyone.at[me], send_sems.at[shift], receive_sems.at[shift],
            device_id=peer(shift),
            device_id_type=pl.DeviceIdType.MESH,
        )
        for shift in range(1, count)
    ]
    for copy in copies:
        copy.start()
    everyone[pl.ds(me, 1)] = mine[...][None]
    for copy in copies:
        copy.wait()


def gather(mine, count, inner):
    vmem = pl.BlockSpec(memory_space=pltpu.VMEM)
    return pl.pallas_call(
        functools.partial(gather_kernel, inner),
        out_shape=jax.ShapeDtypeStruct((count,) + mine.shape, mine.dtype),
        in_specs=[vmem],
        out_specs=vmem,
        scratch_shapes=[pltpu.SemaphoreType.DMA((count,)), pltpu.SemaphoreType.DMA((count,))],
        compiler_params=pltpu.CompilerParams(collective_id=0, has_side_effects=True),
        name="gather",
    )(mine)


def on_device(photons, halo_cells, halo_counts, owners, density):
    rows_x, rows_y, grid = density.shape
    slots = photons.shape[1]
    count_x = lax.axis_size("px")
    count_h, count_l = lax.axis_size("ph"), lax.axis_size("pl")
    count_y = count_h * count_l
    place_x, place_h, place_l = (lax.axis_index(name) for name in ("px", "ph", "pl"))
    place_y = place_h * count_l + place_l
    devices_all = count_x * count_y
    planes = grid // devices_all
    area = rows_x * rows_y
    table_np = hartley(grid)
    table = jnp.asarray(table_np)
    table_x = table.reshape(count_x, rows_x, grid)
    table_y = table.reshape(count_y, rows_y, grid)

    first = max(1, planes * 2 // 3)
    assert first < planes
    parts = [(0, first), (first, planes)]
    shared = np.arange(grid).reshape(count_x, count_h, count_l, planes)[..., first:]
    shared = shared.transpose(0, 2, 1, 3).reshape(count_x, count_l, -1)
    by_plane = table_np.reshape(grid, devices_all, planes)
    tables = [by_plane[:, :, a:b].reshape(grid, devices_all * (b - a)) for a, b in parts]

    pair = LANES // 2
    width = pair // count_x
    assert rows_x % 2 == 0
    assert 2 * grid <= 1 << TAB_BITS and rows_x * grid * grid < 1 << 24
    half_x = rows_x // 2
    rows = grid * half_x
    slot_index = jnp.arange(slots, dtype=jnp.int32)[None, :]
    live = slot_index < halo_counts[:, None]
    weights = jnp.where(live, photons, 0.0)
    cell_x = halo_cells // (rows_y * grid)
    cell_y = owners * rows_y + halo_cells // grid % rows_y
    cell_z = halo_cells % grid
    row = (cell_x // 2) * grid + cell_y
    key = jnp.where(live, row * (2 * grid) + (cell_x % 2) * grid + cell_z, 0)
    sent = jnp.concatenate([weights, key.astype(jnp.float32)])
    slab = gather(sent, count_y, count_l).reshape(count_y, 2, -1, slots)
    slab = [slab[:, kind].reshape(-1, slots) for kind in range(2)]
    slab, density = lax.optimization_barrier((slab, density))

    def signed(index_values):
        return jnp.where(index_values < grid // 2, index_values, index_values - grid).astype(
            jnp.float32
        )

    received = []

    def exchange(blocks_out, among=("px", "ph", "pl")):
        blocks_out = blocks_out.reshape(lax.axis_size(among), -1, LANES)
        if received:
            blocks_out, _ = lax.optimization_barrier((blocks_out, received[-1]))
        got = lax.all_to_all(
            blocks_out, among, split_axis=0, concat_axis=0, tiled=True
        )
        received.append(got)
        return got

    specs = [spread(density, part) for part in tables]
    density_got = [exchange(specs[0])]

    freq = signed(jnp.arange(grid, dtype=jnp.int32))
    freq_z = signed(
        (place_x * count_y + place_y) * planes + jnp.arange(planes, dtype=jnp.int32)
    )
    shared_z = signed(jnp.asarray(shared, dtype=jnp.int32)[place_x, place_l])

    def window_of(freq_z):
        return lax.optimization_barrier(
            top_hat(freq_z[:, None, None], freq[None, :, None], freq[None, None, :], grid)
        )

    rest = window_of(jnp.concatenate([freq_z[first:], shared_z]))
    windows = [window_of(freq_z[:first]), rest[: planes - first]]
    shared_window = rest[planes - first :]

    all_keys = slab[1].astype(jnp.int32)
    all_keys = all_keys // (2 * grid) * (1 << TAB_BITS) + all_keys % (2 * grid)
    all_counts = jnp.max(jnp.where(slab[0] != 0.0, slot_index + 1, 0), axis=1)
    alone = np.arange(grid).reshape(count_x, count_y, planes)[..., :first]
    columns = np.concatenate(
        [
            alone.transpose(1, 0, 2),
            np.tile(shared.transpose(1, 0, 2), (count_h, 1, 1)),
        ],
        axis=2,
    )
    used = columns.shape[2]
    assert used <= width
    own = np.zeros((count_y, grid, count_x, width), np.float32)
    own[..., :used] = table_np[:, columns].transpose(1, 0, 2, 3)
    own = jnp.asarray(own.reshape(count_y, grid, pair))[place_y]
    waves = jnp.concatenate(
        [jnp.pad(own, ((0, 0), (0, pair))), jnp.pad(own, ((0, 0), (pair, 0)))]
    )
    painted = paint(all_keys, slab[0], all_counts, waves, rows)
    for spec in specs[1:]:
        spec, painted = lax.optimization_barrier((spec, painted))
        density_got.append(exchange(spec))

    half_y = lax.dynamic_index_in_dim(
        table_y.reshape(count_h, count_l, rows_y, grid), place_h, 0, keepdims=False
    )

    def rows_back(full, sums_y):
        half = product("kmn,qlm->qkln", full, sums_y)
        return product("qkln,ixn->iqklx", half, table_x)

    def outward(full):
        return exchange(rows_back(full, table_y))

    def inward(got):
        got = got.reshape(count_x, count_y, -1, rows_y, rows_x)
        half = product("iqklx,ixn->qkln", got, table_x)
        return product("qkln,qlm->kmn", half, table_y)

    lines = product("ayc,ym->acm", painted.reshape(half_x, grid, LANES), table)
    lines = lines.reshape(rows_x, count_x, width, grid)[:, :, :used]
    lines = lines.transpose(1, 2, 0, 3)
    rows_of = [
        lax.dynamic_index_in_dim(table_x, (place_x - shift) % count_x, 0, keepdims=False)
        for shift in range(count_x)
    ]
    photon_parts = [
        [
            lax.dynamic_slice(
                lines, ((place_x + shift) % count_x, a, 0, 0), (1, b - a, rows_x, grid)
            )[0]
            for shift in range(count_x)
        ]
        for a, b in ((0, first), (first, used))
    ]

    def around(block, shift):
        if shift == 0:
            return block
        return lax.ppermute(block, "px", [(i, (i + shift) % count_x) for i in range(count_x)])

    photon_parts = [
        [around(block, shift) for shift, block in enumerate(blocks)]
        for blocks in photon_parts
    ]

    def crosswise(blocks):
        total = None
        for block, rows_from in zip(blocks, rows_of):
            term = product("kxm,xn->kmn", block, rows_from)
            total = term if total is None else total + term
        return total

    density_back = [outward(inward(got) * win) for got, win in zip(density_got, windows)]
    across = crosswise(photon_parts[0])
    photon_first = outward(across * windows[0])

    def backward(got):
        total = None
        for part, waves in zip(got, tables):
            term = product("ka,zk->az", part.reshape(-1, area), jnp.asarray(waves))
            total = term if total is None else total + term
        return total

    density_smooth = backward(density_back)
    last = rows_back(crosswise(photon_parts[1]) * shared_window, half_y)
    last, density_smooth = lax.optimization_barrier((last, density_smooth))
    photon_last = exchange(last, ("px", "pl"))
    photon_smooth = backward([photon_first])
    return finish(
        photon_last, photon_smooth, density_smooth, table_np[:, shared.reshape(-1)], rows_x, rows_y
    )


def solution(mesh):
    devices = mesh.devices
    count_x, count_y = devices.shape
    inner = jax.sharding.Mesh(devices.reshape(count_x, 2, count_y // 2), ("px", "ph", "pl"))
    every, split = ("px", "ph", "pl"), ("ph", "pl")
    placed = (P(every, None), P(every, None), P(every), P(every, None), P("px", split, None))

    return jax.shard_map(
        on_device, mesh=inner, in_specs=placed, out_specs=P("px", split, None), check_vma=False
    )
```
